32 devices in a mesh: dp: 2 (over x), expert: 16 (over z, y, core).
Axes of the slice: x: 2, y: 2, z: 4, core: 2. Of those that a mesh axis runs over, the one named last changes fastest.
Arguments:
- gradients: bfloat16 [16, 1024, 5888], P(None, ('dp', 'expert')), may hold values from -6 to 6
- momentum: bfloat16 [16, 1024, 5888], P('expert', 'dp'), may hold values from -6 to 6
- right_factor: bfloat16 [16, 5888, 256], P('expert', 'dp'), may hold values from -6 to 6
Outputs:
- new_momentum: bfloat16 [16, 1024, 5888], P('expert', 'dp')
- new_factor: bfloat16 [16, 5888, 256], P('expert', 'dp')
- update_rows: bfloat16 [16, 1024, 5888], P(None, ('dp', 'expert'))
The draws below stay inside these ranges and needn't reach their ends.
All inputs are finite; a program needn't handle non-finite values.
Results may differ from the reference program's by a relative error of at most 0.009.
Values may be sent and summed in bfloat16 or wider, within the bound.
A program may use at most 128 MiB of HBM per device.

```python
import math
import jax
import jax.numpy as jnp
from jax import lax

D = 5888
FFW = 1024
RANK = 256
EXPERTS = 16


def levels(own_key, dims, pieces, smallest, top_value):
    gain = 1.0
    for dim, blocks in pieces:
        heights = jax.random.uniform(jax.random.fold_in(jax.random.fold_in(own_key, 6), dim), (blocks,), jnp.float32, smallest / len(pieces), top_value / len(pieces))
        gain = gain * jnp.repeat(jnp.exp(heights), dims[dim] // blocks).reshape((-1,) + (1,) * (len(dims) - 1 - dim))
    return gain


def scatter_about(own_key, dims, width, limit, pieces=(), kind=jnp.bfloat16):
    array = width * jax.random.normal(own_key, dims, jnp.float32)
    if pieces:
        array = array * levels(own_key, dims, pieces, -0.22, 0.18)
    return jnp.clip(array, -limit, limit).astype(kind)


def setup_inputs(seed: int = 0) -> dict:
    arg_keys = jax.random.split(jax.random.key(seed), 4)
    return {
        "gradients": scatter_about(arg_keys[0], (EXPERTS, FFW, D), 1.0, 6.0, ((1, 32),)),
        "momentum": scatter_about(arg_keys[1], (EXPERTS, FFW, D), 1.0, 6.0, ((0, 16), (1, 2))),
        "right_factor": scatter_about(arg_keys[2], (EXPERTS, D, RANK), 1.0, 6.0, ((0, 16), (1, 2))),
    }


decay_rate = 0.95
epsilon = 1e-06

def one_expert(items):
    grad_rows, moment_rows, factor = items
    blended = (decay_rate * moment_rows.astype(jnp.float32) + grad_rows.astype(jnp.float32)).astype(jnp.bfloat16)
    left = jnp.dot(blended.astype(jnp.float32), factor.astype(jnp.float32), preferred_element_type=jnp.float32)
    gram_matrix = jnp.dot(left.T, left, precision=lax.Precision.HIGHEST)
    lower = jnp.linalg.cholesky(gram_matrix)
    inverse = jax.scipy.linalg.solve_triangular(lower, jnp.eye(RANK, dtype=jnp.float32), lower=True)
    ortho = jnp.dot(left, inverse.T, precision=lax.Precision.HIGHEST).astype(jnp.bfloat16)
    right = lax.dot_general(blended.astype(jnp.float32), ortho.astype(jnp.float32), (((0,), (0,)), ((), ())), preferred_element_type=jnp.float32)
    right_rounded = right.astype(jnp.bfloat16)
    kept = (blended.astype(jnp.float32) - (1.0 - decay_rate) * lax.dot_general(ortho.astype(jnp.float32), right_rounded.astype(jnp.float32), (((1,), (1,)), ((), ())), preferred_element_type=jnp.float32)).astype(jnp.bfloat16)
    column = lax.optimization_barrier(jnp.sum(right * right, axis=0))
    new_factor = (right * lax.rsqrt(column / D + epsilon)).astype(jnp.bfloat16)
    update = (math.sqrt(FFW / RANK) * lax.dot_general(ortho.astype(jnp.float32), new_factor.astype(jnp.float32), (((1,), (1,)), ((), ())), preferred_element_type=jnp.float32)).astype(jnp.bfloat16)
    return (kept, new_factor, update)

def reference(gradients, momentum, right_factor):
    kept, new_factor, update = lax.map(one_expert, (gradients, momentum, right_factor))
    return (kept, new_factor, update)
```

```python
import math

import jax
import jax.numpy as jnp
from jax import lax
from jax.sharding import PartitionSpec as P

decay_rate = 0.95
epsilon = 1e-06
CHUNKS = 2


def make_body(dp):
    def others(value, wire=None):
        sent = value if wire is None else value.astype(wire)
        for step in range(1, dp):
            yield step, lax.ppermute(sent, "dp", [(i, (i + step) % dp) for i in range(dp)])

    def body(gradients, momentum, right_factor):
        place = lax.axis_index("dp")
        experts = gradients.shape[0]
        rows, width = momentum.shape[1], momentum.shape[2]
        depth, rank = right_factor.shape[1], right_factor.shape[2]
        factor = jnp.zeros((dp * depth, rank), right_factor.dtype)
        factor = lax.dynamic_update_slice(factor, right_factor[0], (place * depth, 0))
        for step, block in others(right_factor[0]):
            factor = lax.dynamic_update_slice(factor, block, ((place - step) % dp * depth, 0))
        arrived = lax.all_to_all(gradients, "expert", split_axis=0, concat_axis=0, tiled=True)
        arrived = arrived.reshape(rows, width)
        blended = (
            decay_rate * momentum[0].astype(jnp.float32) + arrived.astype(jnp.float32)
        ).astype(jnp.bfloat16)
        left = jnp.dot(blended, factor, preferred_element_type=jnp.float32)
        gram = jnp.dot(left.T, left, precision=lax.Precision.HIGHEST)
        gram_matrix = gram
        for _, block in others(gram):
            gram_matrix = gram_matrix + block
        lower = jnp.linalg.cholesky(gram_matrix)
        inverse = jax.scipy.linalg.solve_triangular(
            lower, jnp.eye(rank, dtype=jnp.float32), lower=True
        )
        ortho = jnp.dot(left, inverse.T, precision=lax.Precision.HIGHEST).astype(jnp.bfloat16)
        pieces = CHUNKS if width % (128 * CHUNKS) == 0 else 1
        size = width // pieces
        rights = []
        for k in range(pieces):
            part = lax.dot_general(
                blended[:, k * size : (k + 1) * size],
                ortho,
                (((0,), (0,)), ((), ())),
                preferred_element_type=jnp.float32,
            )
            total = part
            for _, block in others(part, jnp.bfloat16):
                total = total + block.astype(jnp.float32)
            rights.append(total)
        right = jnp.concatenate(rights, axis=0)
        column = jnp.sum(right * right, axis=0)
        new_factor = (right * lax.rsqrt(column / width + epsilon)).astype(jnp.bfloat16)
        update = (
            math.sqrt(rows * dp / rank)
            * lax.dot_general(
                ortho, new_factor, (((1,), (1,)), ((), ())), preferred_element_type=jnp.float32
            )
        ).astype(jnp.bfloat16)
        returned = lax.all_to_all(
            update.reshape(experts, rows // experts, width),
            "expert",
            split_axis=0,
            concat_axis=0,
            tiled=True,
        )
        kept = (
            blended.astype(jnp.float32)
            - (1.0 - decay_rate)
            * lax.dot_general(
                ortho,
                right.astype(jnp.bfloat16),
                (((1,), (1,)), ((), ())),
                preferred_element_type=jnp.float32,
            )
        ).astype(jnp.bfloat16)
        own_factor = lax.dynamic_slice(new_factor, (place * depth, 0), (depth, rank))
        return kept[None], own_factor[None], returned

    return body


def solution(mesh):
    in_specs = (P(None, ("dp", "expert"), None), P("expert", "dp", None), P("expert", "dp", None))
    out_specs = (P("expert", "dp", None), P("expert", "dp", None), P(None, ("dp", "expert"), None))
    return jax.shard_map(
        make_body(mesh.shape["dp"]),
        mesh=mesh,
        in_specs=in_specs,
        out_specs=out_specs,
        check_vma=False,
    )
```

```python
import functools
import math

import jax
import jax.numpy as jnp
from jax import lax
from jax.experimental import pallas as pl
from jax.experimental.pallas import tpu as pltpu
from jax.sharding import PartitionSpec as P

MESH = pl.DeviceIdType.MESH

decay_rate = 0.95
epsilon = 1e-06
CHUNKS = 2


def exchange_kernel(groups, size, src, dst, via_up, via_down, hold, sems):
    count = groups * size
    me = lax.axis_index("expert")
    group, seat = me // size, me % size
    half = src.shape[2] // 2

    def device(step, shift):
        return lax.rem(group + step, groups) * size + lax.rem(seat + shift, size)

    def send(source, target, slot, peer):
        return pltpu.make_async_remote_copy(
            src_ref=source,
            dst_ref=target,
            send_sem=sems.at[0, slot],
            recv_sem=sems.at[1, slot],
            device_id={"expert": peer},
            device_id_type=MESH,
        )

    barrier = pltpu.get_barrier_semaphore()

    @pl.loop(1, count)
    def _(step):
        pl.semaphore_signal(
            barrier, inc=1, device_id={"expert": lax.rem(me + step, count)}, device_id_type=MESH
        )

    pl.semaphore_wait(barrier, count - 1)

    own_in = pltpu.make_async_copy(src.at[me], hold, sems.at[0, 0])
    own_in.start()
    first, second, slot = [], [], 1
    for k in range(size):
        far = device(2, k)
        up = send(src.at[far, :, pl.ds(0, half)], via_up.at[k], slot, device(1, 0))
        down = send(src.at[far, :, pl.ds(half, half)], via_down.at[k], slot + 1, device(3, 0))
        up.start()
        down.start()
        first += [up, down]
        slot += 2
    for k in range(size):
        for step in (1, 3, 0):
            if step == 0 and k == 0:
                continue
            copy = send(src.at[device(step, k)], dst.at[me], slot, device(step, k))
            copy.start()
            second.append(copy)
            slot += 1
    own_in.wait()
    own_out = pltpu.make_async_copy(hold, dst.at[me], sems.at[0, 0])
    own_out.start()
    for k in range(size):
        first[2 * k].wait_recv()
        up = send(via_up.at[k], dst.at[device(3, 0), :, pl.ds(0, half)], slot, device(1, k))
        up.start()
        first[2 * k + 1].wait_recv()
        down = send(
            via_down.at[k], dst.at[device(1, 0), :, pl.ds(half, half)], slot + 1, device(3, k)
        )
        down.start()
        second += [up, down]
        slot += 2
    for copy in first:
        copy.wait_send()
    for copy in second:
        copy.wait()
    own_out.wait()


def exchange(blocks, n, identity):
    count, rows, width = blocks.shape
    if n % 4 or count != n or width % 256:
        return lax.all_to_all(blocks, "expert", split_axis=0, concat_axis=0, tiled=True)
    groups, size = 4, n // 4
    return pl.pallas_call(
        functools.partial(exchange_kernel, groups, size),
        out_shape=jax.ShapeDtypeStruct(blocks.shape, blocks.dtype),
        in_specs=[pl.BlockSpec(memory_space=pl.ANY)],
        out_specs=pl.BlockSpec(memory_space=pl.ANY),
        scratch_shapes=[
            pltpu.VMEM((size, rows, width // 2), blocks.dtype),
            pltpu.VMEM((size, rows, width // 2), blocks.dtype),
            pltpu.VMEM((rows, width), blocks.dtype),
            pltpu.SemaphoreType.DMA((2, 7 * size)),
        ],
        compiler_params=pltpu.CompilerParams(collective_id=identity, has_side_effects=True),
        cost_estimate=pl.CostEstimate(flops=0, bytes_accessed=250_000_000, transcendentals=0),
        name=f"exchange_{identity}",
    )(blocks)


def inverse_kernel(lower_ref, out_ref):
    lower = lower_ref[...]
    rank = lower.shape[0]
    row = lax.broadcasted_iota(jnp.int32, lower.shape, 0)
    col = lax.broadcasted_iota(jnp.int32, lower.shape, 1)
    diagonal = jnp.sum(jnp.where(row == col, lower, 0.0), axis=1, keepdims=True)
    result = jnp.where(row == col, 1.0 / diagonal, 0.0)
    size = 1
    while size < rank:
        inside = (row // (2 * size) == col // (2 * size)) & (row // size > col // size)
        below = jnp.where(inside, lower, 0.0)
        product = jnp.dot(below, result, precision=lax.Precision.HIGHEST)
        result = result - jnp.dot(result, product, precision=lax.Precision.HIGHEST)
        size *= 2
    out_ref[...] = result


def invert(lower):
    return pl.pallas_call(
        inverse_kernel,
        out_shape=jax.ShapeDtypeStruct(lower.shape, lower.dtype),
        in_specs=[pl.BlockSpec(memory_space=pltpu.VMEM)],
        out_specs=pl.BlockSpec(memory_space=pltpu.VMEM),
        name="triangular_inverse",
    )(lower)


def make_body(dp, n):
    def others(value, wire=None):
        sent = value if wire is None else value.astype(wire)
        for step in range(1, dp):
            yield step, lax.ppermute(sent, "dp", [(i, (i + step) % dp) for i in range(dp)])

    def body(gradients, momentum, right_factor):
        place = lax.axis_index("dp")
        rows, width = momentum.shape[1], momentum.shape[2]
        depth, rank = right_factor.shape[1], right_factor.shape[2]
        factor = jnp.zeros((dp * depth, rank), right_factor.dtype)
        factor = lax.dynamic_update_slice(factor, right_factor[0], (place * depth, 0))
        for step, block in others(right_factor[0]):
            factor = lax.dynamic_update_slice(factor, block, ((place - step) % dp * depth, 0))
        arrived = exchange(gradients, n, 1)
        arrived = arrived.reshape(rows, width)
        blended = (
            decay_rate * momentum[0].astype(jnp.float32) + arrived.astype(jnp.float32)
        ).astype(jnp.bfloat16)
        left = jnp.dot(blended, factor, preferred_element_type=jnp.float32)
        gram = jnp.dot(left.T, left, precision=lax.Precision.HIGHEST)
        gram_matrix = gram
        for _, block in others(gram):
            gram_matrix = gram_matrix + block
        lower = jnp.linalg.cholesky(gram_matrix)
        inverse = invert(lower)
        ortho = jnp.dot(left, inverse.T, precision=lax.Precision.HIGHEST).astype(jnp.bfloat16)
        pieces = CHUNKS if width % (128 * CHUNKS) == 0 else 1
        size = width // pieces
        rights = []
        for k in range(pieces):
            part = lax.dot_general(
                blended[:, k * size : (k + 1) * size],
                ortho,
                (((0,), (0,)), ((), ())),
                preferred_element_type=jnp.float32,
            )
            total = part
            for _, block in others(part, jnp.bfloat16):
                total = total + block.astype(jnp.float32)
            rights.append(total)
        right = jnp.concatenate(rights, axis=0)
        column = jnp.sum(right * right, axis=0)
        new_factor = (right * lax.rsqrt(column / width + epsilon)).astype(jnp.bfloat16)
        update = (
            math.sqrt(rows * dp / rank)
            * lax.dot_general(
                ortho, new_factor, (((1,), (1,)), ((), ())), preferred_element_type=jnp.float32
            )
        ).astype(jnp.bfloat16)
        returned = exchange(update.reshape(n, rows // n, width), n, 2)
        kept = (
            blended.astype(jnp.float32)
            - (1.0 - decay_rate)
            * lax.dot_general(
                ortho,
                right.astype(jnp.bfloat16),
                (((1,), (1,)), ((), ())),
                preferred_element_type=jnp.float32,
            )
        ).astype(jnp.bfloat16)
        own_factor = lax.dynamic_slice(new_factor, (place * depth, 0), (depth, rank))
        return kept[None], own_factor[None], returned

    return body


def solution(mesh):
    in_specs = (P(None, ("dp", "expert"), None), P("expert", "dp", None), P("expert", "dp", None))
    out_specs = (P("expert", "dp", None), P("expert", "dp", None), P(None, ("dp", "expert"), None))
    return jax.shard_map(
        make_body(mesh.shape["dp"], mesh.shape["expert"]),
        mesh=mesh,
        in_specs=in_specs,
        out_specs=out_specs,
        check_vma=False,
    )
```

```python
import math

import jax
import jax.numpy as jnp
from jax import lax
from jax.experimental import pallas as pl
from jax.experimental.pallas import tpu as pltpu
from jax.sharding import PartitionSpec as P

decay_rate = 0.95
epsilon = 1e-06
CHUNKS = 2


def dot(a, b, contract=(1, 0)):
    return lax.dot_general(
        a,
        b,
        (((contract[0],), (contract[1],)), ((), ())),
        precision=lax.Precision.HIGHEST,
        preferred_element_type=jnp.float32,
    )


def inverted(lower):
    rank = lower.shape[0]
    row = lax.broadcasted_iota(jnp.int32, lower.shape, 0)
    col = lax.broadcasted_iota(jnp.int32, lower.shape, 1)
    diagonal = jnp.sum(jnp.where(row == col, lower, 0.0), axis=1, keepdims=True)
    result = jnp.where(row == col, 1.0 / diagonal, 0.0)
    size = 1
    while size < rank:
        inside = (row // (2 * size) == col // (2 * size)) & (row // size > col // size)
        below = jnp.where(inside, lower, 0.0)
        result = result - dot(result, dot(below, result))
        size *= 2
    return result


def panel_kernel(lower, gram, inverse, below, rest):
    half = lower.shape[0]
    inverse[...] = inverted(lower[...])
    below[...] = dot(gram[half:, :half], inverse[...], (1, 1))
    rest[...] = gram[half:, half:] - dot(below[...], below[...], (1, 1))


def join_kernel(lower, first, below, out):
    half = lower.shape[0]
    second = inverted(lower[...])
    out[:half, :half] = first[...]
    out[:half, half:] = jnp.zeros_like(second)
    out[half:, :half] = -dot(second, dot(below[...], first[...]))
    out[half:, half:] = second


def cholesky_inverse(gram):
    half = gram.shape[0] // 2
    block = jax.ShapeDtypeStruct((half, half), jnp.float32)
    vmem = pl.BlockSpec(memory_space=pltpu.VMEM)
    lower = lax.linalg.cholesky(gram[:half, :half], symmetrize_input=False)
    first, below, rest = pl.pallas_call(
        panel_kernel,
        out_shape=(block, block, block),
        in_specs=[vmem] * 2,
        out_specs=(vmem, vmem, vmem),
        name="cholesky_panel",
    )(lower, gram)
    lower = lax.linalg.cholesky(rest, symmetrize_input=False)
    return pl.pallas_call(
        join_kernel,
        out_shape=jax.ShapeDtypeStruct(gram.shape, jnp.float32),
        in_specs=[vmem] * 3,
        out_specs=vmem,
        name="cholesky_join",
    )(lower, first, below)


def make_body(dp):
    def others(value, wire=None):
        sent = value if wire is None else value.astype(wire)
        for step in range(1, dp):
            yield step, lax.ppermute(sent, "dp", [(i, (i + step) % dp) for i in range(dp)])

    def body(gradients, momentum, right_factor):
        place = lax.axis_index("dp")
        experts = gradients.shape[0]
        rows, width = momentum.shape[1], momentum.shape[2]
        depth, rank = right_factor.shape[1], right_factor.shape[2]
        factor = jnp.zeros((dp * depth, rank), right_factor.dtype)
        factor = lax.dynamic_update_slice(factor, right_factor[0], (place * depth, 0))
        for step, block in others(right_factor[0]):
            factor = lax.dynamic_update_slice(factor, block, ((place - step) % dp * depth, 0))
        arrived = lax.all_to_all(gradients, "expert", split_axis=0, concat_axis=0, tiled=True)
        arrived = arrived.reshape(rows, width)
        blended = (
            decay_rate * momentum[0].astype(jnp.float32) + arrived.astype(jnp.float32)
        ).astype(jnp.bfloat16)
        left = jnp.dot(blended, factor, preferred_element_type=jnp.float32)
        gram = jnp.dot(left.T, left, precision=lax.Precision.HIGHEST)
        gram_matrix = gram
        for _, block in others(gram):
            gram_matrix = gram_matrix + block
        inverse = cholesky_inverse(gram_matrix)
        ortho = jnp.dot(left, inverse.T, precision=lax.Precision.HIGHEST).astype(jnp.bfloat16)
        pieces = CHUNKS if width % (128 * CHUNKS) == 0 else 1
        size = width // pieces
        rights = []
        for k in range(pieces):
            part = lax.dot_general(
                blended[:, k * size : (k + 1) * size],
                ortho,
                (((0,), (0,)), ((), ())),
                preferred_element_type=jnp.float32,
            )
            total = part
            for _, block in others(part, jnp.bfloat16):
                total = total + block.astype(jnp.float32)
            rights.append(total)
        right = jnp.concatenate(rights, axis=0)
        column = jnp.sum(right * right, axis=0)
        new_factor = (right * lax.rsqrt(column / width + epsilon)).astype(jnp.bfloat16)
        update = (
            math.sqrt(rows * dp / rank)
            * lax.dot_general(
                ortho, new_factor, (((1,), (1,)), ((), ())), preferred_element_type=jnp.float32
            )
        ).astype(jnp.bfloat16)
        returned = lax.all_to_all(
            update.reshape(experts, rows // experts, width),
            "expert",
            split_axis=0,
            concat_axis=0,
            tiled=True,
        )
        kept = (
            blended.astype(jnp.float32)
            - (1.0 - decay_rate)
            * lax.dot_general(
                ortho,
                right.astype(jnp.bfloat16),
                (((1,), (1,)), ((), ())),
                preferred_element_type=jnp.float32,
            )
        ).astype(jnp.bfloat16)
        own_factor = lax.dynamic_slice(new_factor, (place * depth, 0), (depth, rank))
        return kept[None], own_factor[None], returned

    return body


def solution(mesh):
    in_specs = (P(None, ("dp", "expert"), None), P("expert", "dp", None), P("expert", "dp", None))
    out_specs = (P("expert", "dp", None), P("expert", "dp", None), P(None, ("dp", "expert"), None))
    return jax.shard_map(
        make_body(mesh.shape["dp"]),
        mesh=mesh,
        in_specs=in_specs,
        out_specs=out_specs,
        check_vma=False,
    )
```
